8 devices in a mesh: seqs: 1 (over z), states: 8 (over y, x, core).
Axes of the slice: x: 2, y: 2, z: 1, core: 2. Of those that a mesh axis runs over, the one named last changes fastest.
Arguments:
- trans_mat: bfloat16 [16384, 16384], P(None, 'states')
- emit_mat: bfloat16 [16384, 10000], P('states')
- init_prob: float32 [16384], P('states')
- tokens: int32 [64, 32], P('seqs')
- lengths: int32 [64], P('seqs')
Outputs:
- output 1: float32 [64], P('seqs')
- output 2: float32 [64, 16384], P('seqs', 'states')
- output 3: float32 [16384, 2048], P(('seqs', 'states'))
All inputs are finite; a program needn't handle non-finite values.
Results may differ from the reference program's by a relative error of at most 0.001.
Values are sent between devices in bfloat16 or wider.
A program may use at most 1 GiB of HBM per device.

```python
import jax
import jax.numpy as jnp
from jax import lax

K = 16384
V = 10000
B = 64
T = 32
GROUPS = 8
BLOCK_SIZE = K // GROUPS


def setup_inputs(seed: int = 0, part: int = 0) -> dict:
    key = jax.random.key(seed)
    key_trans, key_emit, key_init, key_part = jax.random.split(key, 4)
    part_key = jax.random.fold_in(key_part, part)
    key_tok, key_len = jax.random.split(part_key, 2)
    tile_rows = 512

    def trans_tile(tile_idx):
        logits = 2.0 * jax.random.normal(jax.random.fold_in(key_trans, tile_idx), (tile_rows, K), jnp.float32)
        return jax.nn.softmax(logits, axis=1).astype(jnp.bfloat16)

    def emit_tile(tile_idx):
        logits = 1.5 * jax.random.normal(jax.random.fold_in(key_emit, tile_idx), (tile_rows, V), jnp.float32)
        return jax.nn.softmax(logits, axis=1).astype(jnp.bfloat16)

    tile_ids = jnp.arange(K // tile_rows)
    trans_mat = lax.map(trans_tile, tile_ids).reshape(K, K)
    emit_mat = lax.map(emit_tile, tile_ids).reshape(K, V)
    init_prob = jax.nn.softmax(2.0 * jax.random.normal(key_init, (K,), jnp.float32))
    tokens = jax.random.randint(key_tok, (B, T), 0, V, jnp.int32)
    drawn_len = jax.random.randint(key_len, (B,), 1, T + 1, jnp.int32)
    lengths = jnp.where(jnp.arange(B) == 0, T, drawn_len).astype(jnp.int32)
    return {'trans_mat': trans_mat, 'emit_mat': emit_mat, 'init_prob': init_prob, 'tokens': tokens, 'lengths': lengths}


def reference(trans_mat, emit_mat, init_prob, tokens, lengths):
    def emit_at(step_idx):
        return jnp.take(emit_mat, tokens[:, step_idx], axis=1).T.astype(jnp.float32)

    first_mass = init_prob[None, :] * emit_at(0)
    first_norm = jnp.sum(first_mass, axis=1)
    alpha_first = first_mass / first_norm[:, None]

    def forward_step(alpha_cur, step_idx):
        pred_mass = jnp.dot(alpha_cur.astype(jnp.bfloat16), trans_mat, preferred_element_type=jnp.float32)
        new_mass = pred_mass * emit_at(step_idx)
        norm_sum = jnp.sum(new_mass, axis=1)
        live_mask = step_idx < lengths
        step_scale = jnp.where(live_mask, norm_sum, 1.0)
        alpha_next = jnp.where(live_mask[:, None], new_mass / norm_sum[:, None], alpha_cur)
        return alpha_next, (alpha_cur.astype(jnp.bfloat16), step_scale)

    later_steps = jnp.arange(1, T)
    alpha_last, (alpha_prev, scales) = lax.scan(forward_step, alpha_first, later_steps)
    loglik = jnp.log(first_norm) + jnp.sum(jnp.log(scales), axis=0)

    def backward_step(carry, inputs):
        beta_cur, pair_sum = carry
        step_idx, prev_bf, step_scale = inputs
        live_mask = step_idx < lengths
        weight = jnp.where(live_mask[:, None], emit_at(step_idx) * beta_cur / step_scale[:, None], 0.0).astype(jnp.bfloat16)
        pair_sum = pair_sum + jnp.einsum('bgi,bgj->gij', prev_bf.reshape(B, GROUPS, BLOCK_SIZE).astype(jnp.float32), weight.reshape(B, GROUPS, BLOCK_SIZE).astype(jnp.float32))
        beta_prev = lax.dot_general(weight, trans_mat, (((1,), (1,)), ((), ())), preferred_element_type=jnp.float32)
        beta_prev = beta_prev + jnp.where(live_mask, 0.0, 1.0)[:, None]
        return (beta_prev, pair_sum), None

    start = (jnp.ones((B, K), jnp.float32), jnp.zeros((GROUPS, BLOCK_SIZE, BLOCK_SIZE), jnp.float32))
    (_, pair_sum), _ = lax.scan(backward_step, start, (later_steps, alpha_prev, scales), reverse=True)
    diag_blocks = jnp.moveaxis(jnp.diagonal(trans_mat.reshape(GROUPS, BLOCK_SIZE, GROUPS, BLOCK_SIZE), axis1=0, axis2=2), 2, 0)
    counts = (diag_blocks.astype(jnp.float32) * pair_sum).reshape(K, BLOCK_SIZE)
    return loglik, alpha_last, counts
```

```python
import functools

import jax
import jax.numpy as jnp
from jax import lax
from jax.experimental import pallas as pl
from jax.experimental.pallas import tpu as pltpu
from jax.sharding import PartitionSpec as P

MESH = pl.DeviceIdType.MESH
LANES = 128
TOP = 2.0 ** 90
SLOT = {'P': 0, 'R2': 1, 'R1p': 2, 'R2p': 3, 'D': 4, 'Dp': 5, 'R1': 5, 'O': 5}
SHARED = 5


def run_kernel(steps, seqs, block, trans, emit, init, lens, post, stats_c, stats_g, hist, vout,
               res, full, wq, acc, ef, eb, psend, pown, qbuf, rbuf, vbuf, gcol, msgc, msgg,
               res_sem, shared_sem, e_sem, h_sem, csend, crecv, gsend, grecv,
               ag_send, ag_recv, ps_send, q_recv, q_send, r_recv):
    me = lax.axis_index('states')
    core = lax.rem(me, 2)
    xpos = lax.rem(lax.div(me, 2), 2)
    ypos = lax.div(me, 4)
    xn = me + 2 - 4 * xpos
    yn = me + 4 - 8 * ypos
    flip = 1 - 2 * core
    r1 = xn + core * (yn - xn)
    r2 = yn + core * (xn - yn)
    dg = xn + yn - me
    dev = {'O': me, 'P': me + flip, 'R1': r1, 'R1p': r1 + flip, 'R2': r2, 'R2p': r2 + flip, 'D': dg, 'Dp': dg + flip}
    others = ['P', 'R1', 'R2', 'R1p', 'R2p', 'D', 'Dp']
    chunks = [pl.ds(c * LANES, LANES) for c in range(block // LANES)]
    tile = min(1024, block)
    half = block // 2

    def remote(src, dst, send, recv, target):
        return pltpu.make_async_remote_copy(src_ref=src, dst_ref=dst, send_sem=send, recv_sem=recv,
                                            device_id={'states': target}, device_id_type=MESH)

    barrier = pltpu.get_barrier_semaphore()
    for rel in others:
        pl.semaphore_signal(barrier, inc=1, device_id={'states': dev[rel]}, device_id_type=MESH)
    pl.semaphore_wait(barrier, 7)

    def shared_copies(rel):
        return [pltpu.make_async_copy(trans.at[pl.ds(dev[rel] * block + h * half, half), :],
                                      res.at[SHARED, pl.ds(h * half, half), :], shared_sem.at[h]) for h in range(2)]

    def shared_start(rel):
        for copy in shared_copies(rel):
            copy.start()

    def shared_wait(rel):
        for copy in shared_copies(rel):
            copy.wait()

    def resident(rel):
        return pltpu.make_async_copy(trans.at[pl.ds(dev[rel] * block, block), :], res.at[SLOT[rel]], res_sem.at[SLOT[rel]])

    def emit_f(t):
        return pltpu.make_async_copy(emit.at[t], ef, e_sem.at[0])

    def emit_b(t):
        return pltpu.make_async_copy(emit.at[t], eb, e_sem.at[1])

    def v_out(t):
        return pltpu.make_async_copy(vbuf, vout.at[t - 1], h_sem.at[0])

    def hist_out(k):
        return pltpu.make_async_copy(full.at[me], hist.at[k], h_sem.at[1])

    def msg_copy(buf, send, recv, i):
        return remote(buf.at[me], buf.at[me], send.at[i], recv.at[me], dev[others[i]])

    def msg_arrival(buf, send, recv, i):
        q = dev[others[i]]
        return remote(buf.at[q], buf.at[q], send.at[i], recv.at[q], q)

    def to_row(part, op):
        wide = jnp.concatenate([part] * (LANES // seqs), axis=0)
        return op(jnp.transpose(wide), axis=0, keepdims=True)

    def to_col(row):
        return jnp.transpose(jnp.broadcast_to(row, (LANES, LANES)))[:seqs]

    ag_names = ['O>P', 'O>R1', 'O>R2', 'R1>R2', 'R1>P', 'R2>P', 'D>P']
    lands = {'O>P': 'P', 'O>R1': 'R1', 'O>R2': 'R2', 'R1>R2': 'D', 'R1>P': 'R2p', 'R2>P': 'R1p', 'D>P': 'Dp'}
    ag_index = {'P': 0, 'R1': 1, 'R2': 2, 'D': 3, 'R2p': 4, 'R1p': 5, 'Dp': 6}

    def ag(name):
        what, where = name.split('>')
        src = dev[what]
        return remote(full.at[src], full.at[src], ag_send.at[ag_names.index(name)], ag_recv.at[ag_index[lands[name]]], dev[where])

    def ag_wait(rel):
        src = dev[rel]
        remote(full.at[src], full.at[src], ag_send.at[0], ag_recv.at[ag_index[rel]], src).wait_recv()

    def to_partner(slot):
        return remote(psend, qbuf.at[slot], ps_send, q_recv.at[slot], dev['P'])

    def outward(slot):
        return remote(qbuf.at[slot], rbuf.at[slot], q_send.at[slot], r_recv.at[slot], dev['R2' if slot == 2 else 'R1'])

    def add_to(dst, src):
        for c in chunks:
            dst[:, c] += src[:, c]

    def f_block(rel, first=False):
        @pl.loop(0, block // tile)
        def _(i):
            c = pl.ds(pl.multiple_of(i * tile, tile), tile)
            r = jnp.dot(full[dev[rel]], res[SLOT[rel], :, c], preferred_element_type=jnp.float32)
            if first:
                acc[:, c] = r
            else:
                acc[:, c] += r

    def b_block(rel, dst):
        @pl.loop(0, block // tile)
        def _(i):
            c = pl.ds(pl.multiple_of(i * tile, tile), tile)
            dst[:, c] = lax.dot_general(wq[...], res[SLOT[rel], c, :], (((1,), (1,)), ((), ())), preferred_element_type=jnp.float32)

    def send_norm():
        part = acc[:, chunks[0]]
        for c in chunks[1:]:
            part = part + acc[:, c]
        msgc[me] = jnp.broadcast_to(to_row(part, jnp.sum), (8, LANES))
        for i in range(7):
            msg_copy(msgc, csend, crecv, i).start()

    def take_norm(k):
        for i in range(7):
            msg_arrival(msgc, csend, crecv, i).wait_recv()
        total = msgc[0]
        for d in range(1, 8):
            total = total + msgc[d]
        row = total[0:1]
        stats_c[pl.ds(k, 1), :] = row
        norm = to_col(row)
        live = lens[...] > k
        for c in chunks:
            post[:, c] = jnp.where(live, acc[:, c] / norm, post[:, c])

    shared_start('Dp')
    emit_f(0).start()
    emit_b(steps - 1).start()
    for rel in ('D', 'R2p', 'R1p', 'R2', 'P'):
        resident(rel).start()
    post[...] = jnp.zeros_like(post)
    gcol[...] = jnp.ones_like(gcol)
    stats_g[...] = jnp.ones_like(stats_g)
    qbuf[3] = jnp.zeros((seqs, block), jnp.float32)
    rbuf[1] = jnp.zeros((seqs, block), jnp.float32)
    rbuf[2] = jnp.zeros((seqs, block), jnp.float32)
    emit_f(0).wait()
    for c in chunks:
        acc[:, c] = init[:, c] * ef[:, c].astype(jnp.float32)
    emit_f(1).start()
    shared_wait('Dp')

    @pl.loop(0, steps - 1)
    def _(k):
        t = steps - 1 - k
        both = k < steps - 2

        send_norm()
        take_norm(k)
        for c in chunks:
            full[me, :, c] = post[:, c].astype(jnp.bfloat16)
        for name in ('O>R1', 'O>R2', 'O>P'):
            ag(name).start()
        hist_out(k).start()

        @pl.when(k >= 1)
        def _():
            for slot in range(3):
                outward(slot).wait_send()
            to_partner(3).wait_send()
            remote(rbuf.at[1], rbuf.at[1], q_send.at[1], r_recv.at[1], dev['R1']).wait_recv()
            remote(rbuf.at[2], rbuf.at[2], q_send.at[2], r_recv.at[2], dev['R2']).wait_recv()
            v_out(t + 1).wait()

        emit_b(t).wait()
        live_next = lens[...] > t + 1
        live = lens[...] > t
        rate = TOP / jnp.where(live_next, gcol[...], 1.0)
        dead = jnp.where(live_next, 0.0, 1.0)
        top = jnp.zeros((seqs, LANES), jnp.float32)
        for c in chunks:
            beta = (qbuf[3, :, c] + rbuf[1, :, c]) + rbuf[2, :, c] + dead
            v = eb[:, c].astype(jnp.float32) * beta
            vbuf[:, c] = v
            w = jnp.where(live, v * rate, 0.0)
            top = jnp.maximum(top, w)
            wq[:, c] = w.astype(jnp.bfloat16)
        v_out(t).start()
        emit_b(t - 1).start()

        @pl.when(both)
        def _():
            msgg[me] = jnp.broadcast_to(to_row(top, jnp.max), (8, LANES))
            for i in range(7):
                msg_copy(msgg, gsend, grecv, i).start()
            b_block('Dp', psend)

        shared_start('R1')

        @pl.when(both)
        def _():
            for i in range(7):
                msg_arrival(msgg, gsend, grecv, i).wait_recv()
            peak = msgg[0]
            for d in range(1, 8):
                peak = jnp.maximum(peak, msgg[d])
            stats_g[pl.ds(k, 1), :] = peak[0:1]
            gcol[...] = to_col(peak[0:1])
            to_partner(0).start()

        @pl.when(k == 0)
        def _():
            resident('D').wait()

        @pl.when(both)
        def _():
            b_block('D', pown)
            to_partner(0).wait()
            add_to(qbuf.at[0], pown)
            outward(0).start()

        @pl.when(k == 0)
        def _():
            resident('R2p').wait()

        @pl.when(both)
        def _():
            b_block('R2p', psend)
            to_partner(1).start()

        shared_wait('R1')

        @pl.when(both)
        def _():
            b_block('R1', pown)
            to_partner(1).wait()
            add_to(qbuf.at[1], pown)
            outward(1).start()

        shared_start('O')
        ag_wait('R1')
        ag('R1>R2').start()
        ag('R1>P').start()
        ag_wait('R2')
        ag('R2>P').start()

        @pl.when(k == 0)
        def _():
            for rel in ('R1p', 'R2', 'P'):
                resident(rel).wait()

        @pl.when(both)
        def _():
            b_block('R1p', psend)
            to_partner(2).start()
            b_block('R2', pown)
            to_partner(2).wait()
            add_to(qbuf.at[2], pown)
            b_block('P', psend)
            to_partner(3).start()

        shared_wait('O')

        @pl.when(both)
        def _():
            b_block('O', pown)
            to_partner(3).wait_recv()
            add_to(qbuf.at[3], pown)

        f_block('O', first=True)
        shared_start('R1')
        ag_wait('P')
        f_block('P')

        @pl.when(both)
        def _():
            remote(rbuf.at[0], rbuf.at[0], q_send.at[0], r_recv.at[0], dev['R1']).wait_recv()
            add_to(qbuf.at[2], rbuf.at[0])
            outward(2).start()

        ag_wait('D')
        ag('D>P').start()
        f_block('R2')
        ag_wait('R1p')
        f_block('R1p')
        shared_wait('R1')
        f_block('R1')
        shared_start('Dp')
        ag_wait('R2p')
        f_block('R2p')
        f_block('D')
        ag_wait('Dp')
        shared_wait('Dp')
        f_block('Dp')

        emit_f(k + 1).wait()
        for c in chunks:
            acc[:, c] = acc[:, c] * ef[:, c].astype(jnp.float32)

        @pl.when(k < steps - 2)
        def _():
            emit_f(k + 2).start()

        for name in ag_names:
            ag(name).wait_send()
        hist_out(k).wait()
        for i in range(7):
            msg_copy(msgc, csend, crecv, i).wait_send()

        @pl.when(both)
        def _():
            for i in range(7):
                msg_copy(msgg, gsend, grecv, i).wait_send()

    v_out(1).wait()
    emit_b(0).wait()
    send_norm()
    take_norm(steps - 1)
    for i in range(7):
        msg_copy(msgc, csend, crecv, i).wait_send()


def solution(mesh):
    def local_run(trans_loc, emit_loc, init_loc, tokens_loc, lengths_loc):
        seqs, steps = tokens_loc.shape
        block = trans_loc.shape[1]
        emit_seq = jnp.take(emit_loc, tokens_loc.T, axis=1, mode='clip')
        emit_seq = jnp.transpose(emit_seq, (1, 2, 0))
        lens = jnp.broadcast_to(lengths_loc[:, None], (seqs, LANES))
        f32, bf16 = jnp.float32, jnp.bfloat16
        sd = jax.ShapeDtypeStruct
        vmem = pl.BlockSpec(memory_space=pltpu.VMEM)
        hbm = pl.BlockSpec(memory_space=pl.ANY)
        dma = pltpu.SemaphoreType.DMA
        post, stats_c, stats_g, hist, vout = pl.pallas_call(
            functools.partial(run_kernel, steps, seqs, block),
            out_shape=(sd((seqs, block), f32), sd((steps, LANES), f32), sd((steps, LANES), f32),
                       sd((steps - 1, seqs, block), bf16), sd((steps - 1, seqs, block), f32)),
            in_specs=[hbm, hbm, vmem, vmem],
            out_specs=(vmem, vmem, vmem, hbm, hbm),
            scratch_shapes=[
                pltpu.VMEM((6, block, block), bf16),
                pltpu.VMEM((8, seqs, block), bf16),
                pltpu.VMEM((seqs, block), bf16),
                pltpu.VMEM((seqs, block), f32),
                pltpu.VMEM((seqs, block), bf16),
                pltpu.VMEM((seqs, block), bf16),
                pltpu.VMEM((seqs, block), f32),
                pltpu.VMEM((seqs, block), f32),
                pltpu.VMEM((4, seqs, block), f32),
                pltpu.VMEM((3, seqs, block), f32),
                pltpu.VMEM((seqs, block), f32),
                pltpu.VMEM((seqs, LANES), f32),
                pltpu.VMEM((8, 8, LANES), f32),
                pltpu.VMEM((8, 8, LANES), f32),
                dma((5,)), dma((2,)), dma((2,)), dma((2,)), dma((7,)), dma((8,)), dma((7,)), dma((8,)),
                dma((7,)), dma((7,)), dma, dma((4,)), dma((3,)), dma((3,)),
            ],
            compiler_params=pltpu.CompilerParams(collective_id=0, has_side_effects=True, vmem_limit_bytes=63 * 2 ** 20),
            name='hmm',
        )(trans_loc, emit_seq, init_loc[None, :], lens)

        norm = stats_c[:, :seqs]
        peak = stats_g[:, :seqs]
        log_norm = jnp.log(norm)
        live = jnp.arange(steps)[:, None] < lengths_loc[None, :]
        loglik = jnp.sum(jnp.where(live, log_norm, 0.0), axis=0)
        scales = [None] * steps
        sigma = jnp.ones((seqs,), f32)
        for t in range(steps - 1, 0, -1):
            if t == steps - 1:
                rate = jnp.full((seqs,), TOP, f32)
            else:
                rate = TOP / jnp.where(live[t + 1], peak[steps - 2 - t], 1.0)
            here = sigma / norm[t]
            scales[t] = jnp.where(live[t], here, 0.0)
            sigma = jnp.where(live[t], here / rate, 1.0)
        scale = jnp.stack(scales[1:])
        weights = (vout * scale[:, :, None]).astype(bf16)
        rows = (steps - 1) * seqs
        pair_sum = lax.dot_general(hist.reshape(rows, block), weights.reshape(rows, block), (((0,), (0,)), ((), ())), preferred_element_type=f32)
        diag_block = lax.dynamic_slice_in_dim(trans_loc, lax.axis_index('states') * block, block, axis=0)
        counts = diag_block.astype(f32) * pair_sum
        return loglik, post, counts

    return jax.shard_map(local_run, mesh=mesh, in_specs=(P(None, 'states'), P('states', None), P('states'), P('seqs', None), P('seqs')), out_specs=(P('seqs'), P('seqs', 'states'), P(('seqs', 'states'), None)), check_vma=False)
```

```python
import functools

import jax
import jax.numpy as jnp
from jax import lax
from jax.experimental import pallas as pl
from jax.experimental.pallas import tpu as pltpu
from jax.sharding import PartitionSpec as P

MESH = pl.DeviceIdType.MESH
LANES = 128
SLOT = {'O': 0, 'R2': 1, 'R2p': 2, 'R1p': 3, 'Dp': 4, 'P': 5, 'R1': 5, 'D': 5}
SHARED = 5
PIECES = 4


def run_kernel(steps, seqs, block, trans, emit, init, lens, post, stats_c, hist, whist,
               res, full, wq, acc, ef, eb, psend, pown, qbuf, rbuf, msgc,
               res_sem, shared_sem, e_sem, h_sem, csend, crecv,
               ag_send, ag_recv, ps_send, q_recv, q_send, r_recv, credit):
    me = lax.axis_index('states')
    core = lax.rem(me, 2)
    xpos = lax.rem(lax.div(me, 2), 2)
    ypos = lax.div(me, 4)
    xn = me + 2 - 4 * xpos
    yn = me + 4 - 8 * ypos
    flip = 1 - 2 * core
    r1 = xn + core * (yn - xn)
    r2 = yn + core * (xn - yn)
    dg = xn + yn - me
    dev = {'O': me, 'P': me + flip, 'R1': r1, 'R1p': r1 + flip, 'R2': r2, 'R2p': r2 + flip, 'D': dg, 'Dp': dg + flip}
    others = ['P', 'R1', 'R2', 'R1p', 'R2p', 'D', 'Dp']
    chunks = [pl.ds(c * LANES, LANES) for c in range(block // LANES)]
    half = block // 2
    halves = [pl.ds(h * half, half) for h in range(2)]
    part = block // PIECES
    parts = [pl.ds(p * part, part) for p in range(PIECES)]
    per_part = [[pl.ds(p * part + c * LANES, LANES) for c in range(max(1, part // LANES))] for p in range(PIECES)]

    def remote(src, dst, send, recv, target):
        return pltpu.make_async_remote_copy(src_ref=src, dst_ref=dst, send_sem=send, recv_sem=recv,
                                            device_id={'states': target}, device_id_type=MESH)

    barrier = pltpu.get_barrier_semaphore()
    for rel in others:
        pl.semaphore_signal(barrier, inc=1, device_id={'states': dev[rel]}, device_id_type=MESH)
    pl.semaphore_wait(barrier, 7)

    def shared(rel, h):
        return pltpu.make_async_copy(trans.at[pl.ds(dev[rel] * block + h * half, half), :],
                                     res.at[SHARED, halves[h], :], shared_sem.at[h])

    def shared_start(rel):
        shared(rel, 0).start()
        shared(rel, 1).start()

    def shared_wait(rel):
        shared(rel, 0).wait()
        shared(rel, 1).wait()

    def resident(rel):
        return pltpu.make_async_copy(trans.at[pl.ds(dev[rel] * block, block), :], res.at[SLOT[rel]], res_sem.at[SLOT[rel]])

    def emit_f(t):
        return pltpu.make_async_copy(emit.at[t], ef, e_sem.at[0])

    def emit_b(t):
        return pltpu.make_async_copy(emit.at[t], eb, e_sem.at[1])

    def whist_out(t):
        return pltpu.make_async_copy(wq, whist.at[t - 1], h_sem.at[0])

    def hist_out(k):
        return pltpu.make_async_copy(full.at[me], hist.at[k], h_sem.at[1])

    def norm_msg(i):
        return remote(msgc.at[me], msgc.at[me], csend.at[i], crecv.at[me], dev[others[i]])

    def norm_arrival(i):
        q = dev[others[i]]
        return remote(msgc.at[q], msgc.at[q], csend.at[i], crecv.at[q], q)

    def grant(i, rel):
        pl.semaphore_signal(credit.at[i], inc=1, device_id={'states': dev[rel]}, device_id_type=MESH)

    def to_row(lanes):
        wide = jnp.concatenate([lanes] * (LANES // seqs), axis=0)
        return jnp.sum(jnp.transpose(wide), axis=0, keepdims=True)

    def to_col(row):
        return jnp.transpose(jnp.broadcast_to(row, (LANES, LANES)))[:seqs]

    ag_names = ['O>P', 'O>R1', 'O>R2', 'R1>R2', 'R1>P', 'R2>P', 'D>P']
    lands = {'O>P': 'P', 'O>R1': 'R1', 'O>R2': 'R2', 'R1>R2': 'D', 'R1>P': 'R2p', 'R2>P': 'R1p', 'D>P': 'Dp'}
    ag_index = {'P': 0, 'R1': 1, 'R2': 2, 'D': 3, 'R2p': 4, 'R1p': 5, 'Dp': 6}

    def ag(name, h):
        what, where = name.split('>')
        place = full.at[dev[what], :, halves[h]]
        return remote(place, place, ag_send.at[ag_names.index(name), h], ag_recv.at[ag_index[lands[name]], h], dev[where])

    def ag_wait(rel, h):
        place = full.at[dev[rel], :, halves[h]]
        remote(place, place, ag_send.at[0, h], ag_recv.at[ag_index[rel], h], dev[rel]).wait_recv()

    def ag_pass(h):
        ag_wait('R1', h)
        ag('R1>R2', h).start()
        ag('R1>P', h).start()
        ag_wait('R2', h)
        ag('R2>P', h).start()

    def to_partner(slot, p):
        return remote(psend.at[:, parts[p]], qbuf.at[slot, :, parts[p]], ps_send.at[p], q_recv.at[slot, p], dev['P'])

    def outward(slot, p):
        return remote(qbuf.at[slot, :, parts[p]], rbuf.at[slot, :, parts[p]], q_send.at[slot, p], r_recv.at[slot, p],
                      dev['R2' if slot == 2 else 'R1'])

    def inward(slot, p):
        place = rbuf.at[slot, :, parts[p]]
        remote(place, place, q_send.at[slot, p], r_recv.at[slot, p], dev['R2' if slot == 2 else 'R1']).wait_recv()

    def f_half(rel, h, first=False):
        r = jnp.dot(full[dev[rel], :, halves[h]], res[SLOT[rel], halves[h], :], preferred_element_type=jnp.float32)
        if first:
            acc[...] = r
        else:
            acc[...] += r

    def b_part(rel, p, dst):
        dst[:, parts[p]] = lax.dot_general(wq[...], res[SLOT[rel], parts[p], :], (((1,), (1,)), ((), ())),
                                           preferred_element_type=jnp.float32)

    def send_norm():
        lanes = acc[:, chunks[0]]
        for c in chunks[1:]:
            lanes = lanes + acc[:, c]
        msgc[me] = jnp.broadcast_to(to_row(lanes), (8, LANES))
        for i in range(7):
            norm_msg(i).start()

    def take_norm(k):
        for i in range(7):
            norm_arrival(i).wait_recv()
        total = msgc[0]
        for d in range(1, 8):
            total = total + msgc[d]
        row = total[0:1]
        stats_c[pl.ds(k, 1), :] = row
        norm = to_col(row)
        live = lens[...] > k
        for c in chunks:
            post[:, c] = jnp.where(live, acc[:, c] / norm, post[:, c])

    def send_alpha():
        for c in chunks:
            full[me, :, c] = post[:, c].astype(jnp.bfloat16)
        for h in range(2):
            for name in ('O>R1', 'O>R2', 'O>P'):
                ag(name, h).start()

    def weigh(t):
        norm = to_col(stats_c[pl.ds(t, 1), :])
        live = lens[...] > t
        dead = jnp.where(lens[...] > t + 1, 0.0, 1.0)
        for c in chunks:
            beta = (qbuf[3, :, c] + rbuf[1, :, c]) + rbuf[2, :, c] + dead
            w = eb[:, c].astype(jnp.float32) * beta / norm
            wq[:, c] = jnp.where(live, w, 0.0).astype(jnp.bfloat16)

    resident('O').start()
    emit_f(0).start()
    emit_b(steps - 1).start()
    shared_start('P')
    for rel in ('R2', 'R2p', 'R1p', 'Dp'):
        resident(rel).start()
    post[...] = jnp.zeros_like(post)
    qbuf[3] = jnp.zeros((seqs, block), jnp.float32)
    rbuf[1] = jnp.zeros((seqs, block), jnp.float32)
    rbuf[2] = jnp.zeros((seqs, block), jnp.float32)
    emit_f(0).wait()
    for c in chunks:
        acc[:, c] = init[:, c] * ef[:, c].astype(jnp.float32)
    emit_f(1).start()
    send_norm()
    take_norm(0)
    send_alpha()
    resident('O').wait()

    @pl.loop(0, steps - 1)
    def _(k):
        more = k < steps - 2
        hist_out(k).start()
        f_half('O', 0, first=True)
        f_half('O', 1)
        ag_wait('P', 0)
        ag_wait('P', 1)
        shared_wait('P')
        f_half('P', 0)
        f_half('P', 1)
        shared_start('R1')

        @pl.when(k == 0)
        def _():
            for rel in ('R2', 'R2p', 'R1p', 'Dp'):
                resident(rel).wait()

        ag_pass(0)
        f_half('R2', 0)
        ag_wait('R2p', 0)
        f_half('R2p', 0)
        ag_wait('R1p', 0)
        f_half('R1p', 0)
        shared_wait('R1')
        f_half('R1', 0)
        ag_pass(1)
        f_half('R1', 1)
        shared_start('D')
        f_half('R2', 1)
        ag_wait('D', 0)
        ag('D>P', 0).start()
        ag_wait('R2p', 1)
        f_half('R2p', 1)
        ag_wait('R1p', 1)
        f_half('R1p', 1)
        ag_wait('Dp', 0)
        f_half('Dp', 0)
        ag_wait('D', 1)
        ag('D>P', 1).start()
        shared_wait('D')
        f_half('D', 0)
        f_half('D', 1)

        @pl.when(more)
        def _():
            shared_start('P')

        emit_f(k + 1).wait()
        ag_wait('Dp', 1)
        f_half('Dp', 1)
        for c in chunks:
            acc[:, c] = acc[:, c] * ef[:, c].astype(jnp.float32)

        for name in ag_names:
            for h in range(2):
                ag(name, h).wait_send()
        hist_out(k).wait()
        for i in range(7):
            norm_msg(i).wait_send()
        send_norm()

        @pl.when(more)
        def _():
            emit_f(k + 2).start()

        take_norm(k + 1)

        @pl.when(more)
        def _():
            send_alpha()

    for i in range(7):
        norm_msg(i).wait_send()

    @pl.loop(0, steps - 2)
    def _(m):
        t = steps - 1 - m
        emit_b(t).wait()

        @pl.when(m >= 1)
        def _():
            whist_out(t + 1).wait()
            for p in range(PIECES):
                for slot in range(3):
                    outward(slot, p).wait_send()
                to_partner(3, p).wait_send()
                inward(1, p)
                inward(2, p)

        weigh(t)
        for i, rel in enumerate(('P', 'R1', 'R2')):
            grant(i, rel)
        whist_out(t).start()
        emit_b(t - 1).start()

        for slot, (far, near) in enumerate((('Dp', 'D'), ('R2p', 'R1'), ('R1p', 'R2'), ('P', 'O'))):
            for kind, p in ((0, 0), (0, 1), (0, 2), (1, 0), (0, 3), (1, 1), (1, 2), (1, 3)):
                if kind == 0:
                    if slot > 0:
                        to_partner(slot - 1, p).wait_send()
                    if slot == 3 and p == 0:
                        shared_wait('P')
                    b_part(far, p, psend)
                    if slot == 0 and p == 0:
                        pl.semaphore_wait(credit.at[0], 1)
                    to_partner(slot, p).start()
                    if slot == 3 and p == PIECES - 1:
                        shared_start('D')
                    continue
                if slot == 0 and p == 0:
                    @pl.when(m >= 1)
                    def _():
                        shared_wait('D')
                if slot == 1 and p == 0:
                    shared_wait('R1')
                b_part(near, p, pown)
                if slot < 2 and p == PIECES - 1:
                    shared_start('R1' if slot == 0 else 'P')
                to_partner(slot, p).wait_recv()
                if slot == 2:
                    inward(0, p)
                for c in per_part[p]:
                    if slot == 2:
                        qbuf[slot, :, c] = (qbuf[slot, :, c] + pown[:, c]) + rbuf[0, :, c]
                    else:
                        qbuf[slot, :, c] += pown[:, c]
                if slot < 3:
                    if p == 0 and slot != 1:
                        pl.semaphore_wait(credit.at[1 if slot == 0 else 2], 1)
                    outward(slot, p).start()

    emit_b(1).wait()
    whist_out(2).wait()
    for p in range(PIECES):
        for slot in range(3):
            outward(slot, p).wait_send()
        to_partner(3, p).wait_send()
        inward(1, p)
        inward(2, p)
    shared_wait('D')
    weigh(1)
    whist_out(1).start()
    whist_out(1).wait()


def solution(mesh):
    def local_run(trans_loc, emit_loc, init_loc, tokens_loc, lengths_loc):
        seqs, steps = tokens_loc.shape
        block = trans_loc.shape[1]
        emit_seq = jnp.take(emit_loc, tokens_loc.T, axis=1, mode='clip')
        emit_seq = jnp.transpose(emit_seq, (1, 2, 0))
        lens = jnp.broadcast_to(lengths_loc[:, None], (seqs, LANES))
        f32, bf16 = jnp.float32, jnp.bfloat16
        sd = jax.ShapeDtypeStruct
        vmem = pl.BlockSpec(memory_space=pltpu.VMEM)
        hbm = pl.BlockSpec(memory_space=pl.ANY)
        dma = pltpu.SemaphoreType.DMA
        post, stats_c, hist, weights = pl.pallas_call(
            functools.partial(run_kernel, steps, seqs, block),
            out_shape=(sd((seqs, block), f32), sd((steps, LANES), f32),
                       sd((steps - 1, seqs, block), bf16), sd((steps - 1, seqs, block), bf16)),
            in_specs=[hbm, hbm, vmem, vmem],
            out_specs=(vmem, vmem, hbm, hbm),
            scratch_shapes=[
                pltpu.VMEM((6, block, block), bf16),
                pltpu.VMEM((8, seqs, block), bf16),
                pltpu.VMEM((seqs, block), bf16),
                pltpu.VMEM((seqs, block), f32),
                pltpu.VMEM((seqs, block), bf16),
                pltpu.VMEM((seqs, block), bf16),
                pltpu.VMEM((seqs, block), f32),
                pltpu.VMEM((seqs, block), f32),
                pltpu.VMEM((4, seqs, block), f32),
                pltpu.VMEM((3, seqs, block), f32),
                pltpu.VMEM((8, 8, LANES), f32),
                dma((5,)), dma((2,)), dma((2,)), dma((2,)), dma((7,)), dma((8,)),
                dma((7, 2)), dma((7, 2)), dma((PIECES,)), dma((4, PIECES)), dma((3, PIECES)), dma((3, PIECES)),
                pltpu.SemaphoreType.REGULAR((3,)),
            ],
            compiler_params=pltpu.CompilerParams(collective_id=0, has_side_effects=True, vmem_limit_bytes=63 * 2 ** 20),
            name='hmm',
        )(trans_loc, emit_seq, init_loc[None, :], lens)

        norm = stats_c[:, :seqs]
        live = jnp.arange(steps)[:, None] < lengths_loc[None, :]
        loglik = jnp.sum(jnp.where(live, jnp.log(norm), 0.0), axis=0)
        rows = (steps - 1) * seqs
        pair_sum = lax.dot_general(hist.reshape(rows, block), weights.reshape(rows, block), (((0,), (0,)), ((), ())), preferred_element_type=f32)
        diag_block = lax.dynamic_slice_in_dim(trans_loc, lax.axis_index('states') * block, block, axis=0)
        counts = diag_block.astype(f32) * pair_sum
        return loglik, post, counts

    return jax.shard_map(local_run, mesh=mesh, in_specs=(P(None, 'states'), P('states', None), P('states'), P('seqs', None), P('seqs')), out_specs=(P('seqs'), P('seqs', 'states'), P(('seqs', 'states'), None)), check_vma=False)
```

```python
import functools

import jax
import jax.numpy as jnp
from jax import lax
from jax.experimental import pallas as pl
from jax.experimental.pallas import tpu as pltpu
from jax.sharding import PartitionSpec as P

MESH = pl.DeviceIdType.MESH
LANES = 128
SLOT = {'O': 0, 'R2': 1, 'R2p': 2, 'R1p': 3, 'Dp': 4, 'P': 5, 'R1': 5, 'D': 5}
SHARED = 5
PIECES = 4


def run_kernel(steps, seqs, block, trans, emit, init, lens, post, stats_c, hist, whist,
               res, full, wq, acc, ef, eb, psend, pown, qbuf, rbuf, msgc,
               res_sem, shared_sem, e_sem, h_sem, csend, crecv,
               ag_send, ag_recv, ps_send, q_recv, q_send, r_recv, credit):
    me = lax.axis_index('states')
    core = lax.rem(me, 2)
    xpos = lax.rem(lax.div(me, 2), 2)
    ypos = lax.div(me, 4)
    xn = me + 2 - 4 * xpos
    yn = me + 4 - 8 * ypos
    flip = 1 - 2 * core
    r1 = xn + core * (yn - xn)
    r2 = yn + core * (xn - yn)
    dg = xn + yn - me
    dev = {'O': me, 'P': me + flip, 'R1': r1, 'R1p': r1 + flip, 'R2': r2, 'R2p': r2 + flip, 'D': dg, 'Dp': dg + flip}
    others = ['P', 'R1', 'R2', 'R1p', 'R2p', 'D', 'Dp']
    chunks = [pl.ds(c * LANES, LANES) for c in range(block // LANES)]
    half = block // 2
    halves = [pl.ds(h * half, half) for h in range(2)]
    cuts = [pl.ds(0, half), pl.ds(half, half // 2), pl.ds(half + half // 2, half // 2)]
    part = block // PIECES
    parts = [pl.ds(p * part, part) for p in range(PIECES)]
    per_part = [[pl.ds(p * part + c * LANES, LANES) for c in range(max(1, part // LANES))] for p in range(PIECES)]

    def remote(src, dst, send, recv, target):
        return pltpu.make_async_remote_copy(src_ref=src, dst_ref=dst, send_sem=send, recv_sem=recv,
                                            device_id={'states': target}, device_id_type=MESH)

    barrier = pltpu.get_barrier_semaphore()
    for rel in others:
        pl.semaphore_signal(barrier, inc=1, device_id={'states': dev[rel]}, device_id_type=MESH)
    pl.semaphore_wait(barrier, 7)

    def shared(rel, h):
        return pltpu.make_async_copy(trans.at[pl.ds(dev[rel] * block + h * half, half), :],
                                     res.at[SHARED, halves[h], :], shared_sem.at[h])

    def shared_start(rel):
        shared(rel, 0).start()
        shared(rel, 1).start()

    def shared_wait(rel):
        shared(rel, 0).wait()
        shared(rel, 1).wait()

    def resident(rel):
        return pltpu.make_async_copy(trans.at[pl.ds(dev[rel] * block, block), :], res.at[SLOT[rel]], res_sem.at[SLOT[rel]])

    def emit_f(t):
        return pltpu.make_async_copy(emit.at[t], ef, e_sem.at[0])

    def emit_b(t):
        return pltpu.make_async_copy(emit.at[t], eb, e_sem.at[1])

    def whist_out(t):
        return pltpu.make_async_copy(wq, whist.at[t - 1], h_sem.at[0])

    def hist_out(k):
        return pltpu.make_async_copy(full.at[me], hist.at[k], h_sem.at[1])

    def norm_msg(i):
        return remote(msgc.at[me], msgc.at[me], csend.at[i], crecv.at[me], dev[others[i]])

    def norm_arrival(i):
        q = dev[others[i]]
        return remote(msgc.at[q], msgc.at[q], csend.at[i], crecv.at[q], q)

    def grant(i, rel):
        pl.semaphore_signal(credit.at[i], inc=1, device_id={'states': dev[rel]}, device_id_type=MESH)

    def to_row(lanes):
        wide = jnp.concatenate([lanes] * (LANES // seqs), axis=0)
        return jnp.sum(jnp.transpose(wide), axis=0, keepdims=True)

    def to_col(row):
        return jnp.transpose(jnp.broadcast_to(row, (LANES, LANES)))[:seqs]

    ag_names = ['O>P', 'O>R1', 'O>R2', 'R1>R2', 'R1>P', 'R2>P', 'D>P']
    lands = {'O>P': 'P', 'O>R1': 'R1', 'O>R2': 'R2', 'R1>R2': 'D', 'R1>P': 'R2p', 'R2>P': 'R1p', 'D>P': 'Dp'}
    ag_index = {'P': 0, 'R1': 1, 'R2': 2, 'D': 3, 'R2p': 4, 'R1p': 5, 'Dp': 6}

    def ag(name, h):
        what, where = name.split('>')
        place = full.at[dev[what], :, cuts[h]]
        return remote(place, place, ag_send.at[ag_names.index(name), h], ag_recv.at[ag_index[lands[name]], h], dev[where])

    def ag_wait(rel, h):
        place = full.at[dev[rel], :, cuts[h]]
        remote(place, place, ag_send.at[0, h], ag_recv.at[ag_index[rel], h], dev[rel]).wait_recv()

    def ag_pass(h):
        ag_wait('R1', h)
        ag('R1>R2', h).start()
        ag('R1>P', h).start()
        ag_wait('R2', h)
        ag('R2>P', h).start()

    def to_partner(slot, p):
        return remote(psend.at[:, parts[p]], qbuf.at[slot, :, parts[p]], ps_send.at[p], q_recv.at[slot, p], dev['P'])

    def outward(slot, p):
        return remote(qbuf.at[slot, :, parts[p]], rbuf.at[slot, :, parts[p]], q_send.at[slot, p], r_recv.at[slot, p],
                      dev['R2' if slot == 2 else 'R1'])

    def inward(slot, p):
        place = rbuf.at[slot, :, parts[p]]
        remote(place, place, q_send.at[slot, p], r_recv.at[slot, p], dev['R2' if slot == 2 else 'R1']).wait_recv()

    def f_half(rel, h, first=False, spans=halves):
        r = jnp.dot(full[dev[rel], :, spans[h]], res[SLOT[rel], spans[h], :], preferred_element_type=jnp.float32)
        if first:
            acc[...] = r
        else:
            acc[...] += r

    def b_part(rel, p, dst):
        dst[:, parts[p]] = lax.dot_general(wq[...], res[SLOT[rel], parts[p], :], (((1,), (1,)), ((), ())),
                                           preferred_element_type=jnp.float32)

    def send_norm():
        lanes = acc[:, chunks[0]]
        for c in chunks[1:]:
            lanes = lanes + acc[:, c]
        msgc[me] = jnp.broadcast_to(to_row(lanes), (8, LANES))
        for i in range(7):
            norm_msg(i).start()

    def take_norm(k):
        for i in range(7):
            norm_arrival(i).wait_recv()
        total = msgc[0]
        for d in range(1, 8):
            total = total + msgc[d]
        row = total[0:1]
        stats_c[pl.ds(k, 1), :] = row
        norm = to_col(row)
        live = lens[...] > k
        for c in chunks:
            post[:, c] = jnp.where(live, acc[:, c] / norm, post[:, c])

    def send_alpha():
        for h in range(3):
            for c in chunks[(0, 4, 6)[h] * len(chunks) // 8:(4, 6, 8)[h] * len(chunks) // 8]:
                full[me, :, c] = post[:, c].astype(jnp.bfloat16)
            for name in ('O>R1', 'O>R2', 'O>P'):
                ag(name, h).start()

    def weigh(t):
        norm = to_col(stats_c[pl.ds(t, 1), :])
        live = lens[...] > t
        dead = jnp.where(lens[...] > t + 1, 0.0, 1.0)
        for c in chunks:
            beta = (qbuf[3, :, c] + rbuf[1, :, c]) + rbuf[2, :, c] + dead
            w = eb[:, c].astype(jnp.float32) * beta / norm
            wq[:, c] = jnp.where(live, w, 0.0).astype(jnp.bfloat16)

    resident('O').start()
    emit_f(0).start()
    emit_b(steps - 1).start()
    shared_start('P')
    for rel in ('R2', 'R2p', 'R1p', 'Dp'):
        resident(rel).start()
    post[...] = jnp.zeros_like(post)
    qbuf[3] = jnp.zeros((seqs, block), jnp.float32)
    rbuf[1] = jnp.zeros((seqs, block), jnp.float32)
    rbuf[2] = jnp.zeros((seqs, block), jnp.float32)
    emit_f(0).wait()
    for c in chunks:
        acc[:, c] = init[:, c] * ef[:, c].astype(jnp.float32)
    emit_f(1).start()
    send_norm()
    take_norm(0)
    send_alpha()
    resident('O').wait()

    @pl.loop(0, steps - 1)
    def _(k):
        more = k < steps - 2
        hist_out(k).start()
        f_half('O', 0, first=True)
        f_half('O', 1)
        for h in range(3):
            ag_wait('P', h)
        shared_wait('P')
        f_half('P', 0)
        f_half('P', 1)
        shared_start('R1')

        @pl.when(k == 0)
        def _():
            for rel in ('R2', 'R2p', 'R1p', 'Dp'):
                resident(rel).wait()

        ag_pass(0)
        f_half('R2', 0)
        ag_wait('R2p', 0)
        f_half('R2p', 0)
        ag_pass(1)
        ag_wait('R1p', 0)
        f_half('R1p', 0)
        shared_wait('R1')
        f_half('R1', 0)
        ag_pass(2)
        f_half('R1', 1)
        shared_start('D')
        f_half('R2', 1)
        ag_wait('D', 0)
        ag('D>P', 0).start()
        ag_wait('R2p', 1)
        ag_wait('R2p', 2)
        f_half('R2p', 1)
        ag_wait('D', 1)
        ag('D>P', 1).start()
        ag_wait('R1p', 1)
        ag_wait('R1p', 2)
        f_half('R1p', 1)
        ag_wait('D', 2)
        ag('D>P', 2).start()
        ag_wait('Dp', 0)
        f_half('Dp', 0)
        shared_wait('D')
        f_half('D', 0)
        f_half('D', 1)

        @pl.when(more)
        def _():
            shared_start('P')

        emit_f(k + 1).wait()
        ag_wait('Dp', 1)
        f_half('Dp', 1, spans=cuts)
        ag_wait('Dp', 2)
        f_half('Dp', 2, spans=cuts)
        for c in chunks:
            acc[:, c] = acc[:, c] * ef[:, c].astype(jnp.float32)

        for name in ag_names:
            for h in range(3):
                ag(name, h).wait_send()
        hist_out(k).wait()
        for i in range(7):
            norm_msg(i).wait_send()
        send_norm()

        @pl.when(more)
        def _():
            emit_f(k + 2).start()

        take_norm(k + 1)

        @pl.when(more)
        def _():
            send_alpha()

    for i in range(7):
        norm_msg(i).wait_send()

    @pl.loop(0, steps - 2)
    def _(m):
        t = steps - 1 - m
        emit_b(t).wait()

        @pl.when(m >= 1)
        def _():
            whist_out(t + 1).wait()
            for p in range(PIECES):
                for slot in range(3):
                    outward(slot, p).wait_send()
                to_partner(3, p).wait_send()
                inward(1, p)
                inward(2, p)

        weigh(t)
        for i, rel in enumerate(('P', 'R1', 'R2')):
            grant(i, rel)
        whist_out(t).start()
        emit_b(t - 1).start()

        for slot, (far, near) in enumerate((('Dp', 'D'), ('R2p', 'R1'), ('R1p', 'R2'), ('P', 'O'))):
            for kind, p in ((0, 0), (0, 1), (0, 2), (1, 0), (0, 3), (1, 1), (1, 2), (1, 3)):
                if kind == 0:
                    if slot > 0:
                        to_partner(slot - 1, p).wait_send()
                    if slot == 3 and p == 0:
                        shared_wait('P')
                    b_part(far, p, psend)
                    if slot == 0 and p == 0:
                        pl.semaphore_wait(credit.at[0], 1)
                    to_partner(slot, p).start()
                    if slot == 3 and p == PIECES - 1:
                        shared_start('D')
                    continue
                if slot == 0 and p == 0:
                    @pl.when(m >= 1)
                    def _():
                        shared_wait('D')
                if slot == 1 and p == 0:
                    shared_wait('R1')
                b_part(near, p, pown)
                if slot < 2 and p == PIECES - 1:
                    shared_start('R1' if slot == 0 else 'P')
                to_partner(slot, p).wait_recv()
                if slot == 2:
                    inward(0, p)
                for c in per_part[p]:
                    if slot == 2:
                        qbuf[slot, :, c] = (qbuf[slot, :, c] + pown[:, c]) + rbuf[0, :, c]
                    else:
                        qbuf[slot, :, c] += pown[:, c]
                if slot < 3:
                    if p == 0 and slot != 1:
                        pl.semaphore_wait(credit.at[1 if slot == 0 else 2], 1)
                    outward(slot, p).start()

    emit_b(1).wait()
    whist_out(2).wait()
    for p in range(PIECES):
        for slot in range(3):
            outward(slot, p).wait_send()
        to_partner(3, p).wait_send()
        inward(1, p)
        inward(2, p)
    shared_wait('D')
    weigh(1)
    whist_out(1).start()
    whist_out(1).wait()


def solution(mesh):
    def local_run(trans_loc, emit_loc, init_loc, tokens_loc, lengths_loc):
        seqs, steps = tokens_loc.shape
        block = trans_loc.shape[1]
        emit_seq = jnp.take(emit_loc, tokens_loc.T, axis=1, mode='clip')
        emit_seq = jnp.transpose(emit_seq, (1, 2, 0))
        lens = jnp.broadcast_to(lengths_loc[:, None], (seqs, LANES))
        f32, bf16 = jnp.float32, jnp.bfloat16
        sd = jax.ShapeDtypeStruct
        vmem = pl.BlockSpec(memory_space=pltpu.VMEM)
        hbm = pl.BlockSpec(memory_space=pl.ANY)
        dma = pltpu.SemaphoreType.DMA
        post, stats_c, hist, weights = pl.pallas_call(
            functools.partial(run_kernel, steps, seqs, block),
            out_shape=(sd((seqs, block), f32), sd((steps, LANES), f32),
                       sd((steps - 1, seqs, block), bf16), sd((steps - 1, seqs, block), bf16)),
            in_specs=[hbm, hbm, vmem, vmem],
            out_specs=(vmem, vmem, hbm, hbm),
            scratch_shapes=[
                pltpu.VMEM((6, block, block), bf16),
                pltpu.VMEM((8, seqs, block), bf16),
                pltpu.VMEM((seqs, block), bf16),
                pltpu.VMEM((seqs, block), f32),
                pltpu.VMEM((seqs, block), bf16),
                pltpu.VMEM((seqs, block), bf16),
                pltpu.VMEM((seqs, block), f32),
                pltpu.VMEM((seqs, block), f32),
                pltpu.VMEM((4, seqs, block), f32),
                pltpu.VMEM((3, seqs, block), f32),
                pltpu.VMEM((8, 8, LANES), f32),
                dma((5,)), dma((2,)), dma((2,)), dma((2,)), dma((7,)), dma((8,)),
                dma((7, 3)), dma((7, 3)), dma((PIECES,)), dma((4, PIECES)), dma((3, PIECES)), dma((3, PIECES)),
                pltpu.SemaphoreType.REGULAR((3,)),
            ],
            compiler_params=pltpu.CompilerParams(collective_id=0, has_side_effects=True, vmem_limit_bytes=63 * 2 ** 20),
            name='hmm',
        )(trans_loc, emit_seq, init_loc[None, :], lens)

        norm = stats_c[:, :seqs]
        live = jnp.arange(steps)[:, None] < lengths_loc[None, :]
        loglik = jnp.sum(jnp.where(live, jnp.log(norm), 0.0), axis=0)
        rows = (steps - 1) * seqs
        pair_sum = lax.dot_general(hist.reshape(rows, block), weights.reshape(rows, block), (((0,), (0,)), ((), ())), preferred_element_type=f32)
        diag_block = lax.dynamic_slice_in_dim(trans_loc, lax.axis_index('states') * block, block, axis=0)
        counts = diag_block.astype(f32) * pair_sum
        return loglik, post, counts

    return jax.shard_map(local_run, mesh=mesh, in_specs=(P(None, 'states'), P('states', None), P('states'), P('seqs', None), P('seqs')), out_specs=(P('seqs'), P('seqs', 'states'), P(('seqs', 'states'), None)), check_vma=False)
```
